128 devices in a mesh: dp: 8 (over y, z_lo), fsdp: 16 (over x, z_hi, core).
Axes of the slice: x: 4, y: 4, z: 4 (z_hi: 2, z_lo: 2; z = z_hi * 2 + z_lo), core: 2. Of those that a mesh axis runs over, the one named last changes fastest.
Arguments:
- latent: bfloat16 [128, 1024, 320], P(('dp', 'fsdp')), may hold values from -6 to 6
- hint: bfloat16 [128, 1024, 320], P(('dp', 'fsdp')), may hold values from -48 to 48
- timestep: int32 [128], P(('dp', 'fsdp')), may hold values from 0 to 999
- skip_grad: bfloat16 [128, 1024, 320], P(('dp', 'fsdp')), may hold values from -6 to 6
- frozen_one: bfloat16 [2880, 320], P('fsdp'), may hold values from -0.109375 to 0.109375
- frozen_two: bfloat16 [2880, 320], P('fsdp'), may hold values from -0.109375 to 0.109375
- time_weight: bfloat16 [320, 1280], P('fsdp'), may hold values from -0.3125 to 0.3125
- frozen_emb: bfloat16 [1280, 320], P('fsdp'), may hold values from -0.15625 to 0.15625
- train_one: bfloat16 [2880, 320], P('fsdp'), may hold values from -0.109375 to 0.109375
- train_two: bfloat16 [2880, 320], P('fsdp'), may hold values from -0.109375 to 0.109375
- train_emb: bfloat16 [1280, 320], P('fsdp'), may hold values from -0.15625 to 0.15625
- zero_weight: bfloat16 [320, 320], P('fsdp'), may hold values from -0.3125 to 0.3125
Outputs:
- skip: bfloat16 [128, 1024, 320], P(('dp', 'fsdp'))
- grad_one: float32 [2880, 320], P('fsdp')
- grad_two: float32 [2880, 320], P('fsdp')
- grad_emb: float32 [1280, 320], P('fsdp')
- grad_zero: float32 [320, 320], P('fsdp')
- grad_norm: float32 [], replicated
The draws below stay inside these ranges and needn't reach their ends.
All inputs are finite; a program needn't handle non-finite values.
Results may differ from the reference program's by a relative error of at most 0.018.
Values may be sent and summed in bfloat16 or wider, within the bound.
A program may use at most 128 MiB of HBM per device.

```python
import math
import jax
import jax.numpy as jnp
from jax import lax

C = 320
TEMB = 1280
COLS = 64
POS = 1024
BATCH = 128


def draw_hint(key, part):
    key = jax.random.fold_in(key, 7311)
    ramp = jnp.arange(C).astype(jnp.float32) / (C - 1)
    scales = jnp.exp(jnp.log(8.0) * ramp)
    noise = jnp.clip(jax.random.normal(key, (BATCH, POS, C), jnp.float32), -6.0, 6.0)
    values = noise * scales[None, None, :]
    return jnp.clip(values, -48.0, 48.0).astype(jnp.bfloat16)


def plant(drawn, key, least, top_value):
    spot = [jax.random.randint(jax.random.fold_in(key, axis), (), 0, length) for axis, length in enumerate(drawn.shape)]
    main_axis = drawn.shape.index(max(drawn.shape))
    next_to = spot[:main_axis] + [(spot[main_axis] + 1) % drawn.shape[main_axis]] + spot[main_axis + 1:]
    return drawn.at[tuple(spot)].set(least).at[tuple(next_to)].set(top_value)


def steps_of(stream_key, dims, cuts, smallest, top_value):
    def one(position, blocks):
        draws = jax.random.uniform(jax.random.fold_in(jax.random.fold_in(stream_key, 6), position), (blocks,), jnp.float32, smallest / len(cuts), top_value / len(cuts))
        return jnp.repeat(jnp.exp(draws), dims[position] // blocks).reshape((-1,) + (1,) * (len(dims) - position - 1))

    factor_of = one(*cuts[0])
    for cut in cuts[1:]:
        factor_of = factor_of * one(*cut)
    return factor_of


def centred(key, extent, deviation, most, pieces=(), kind=jnp.bfloat16):
    factor_of = steps_of(key, extent, pieces, -0.22, 0.18) if pieces else 1.0
    result = jax.random.normal(key, extent, jnp.float32) * deviation * factor_of
    return jnp.minimum(jnp.maximum(result, -most), most).astype(kind)


def setup_inputs(seed: int = 0) -> dict:
    splits = jax.random.split(jax.random.key(seed), 13)
    return {
        "latent": centred(splits[0], (BATCH, POS, C), 1.0, 6.0, ((0, 128),)),
        "hint": draw_hint(jax.random.fold_in(splits[12], 71), 0),
        "timestep": plant(jax.random.randint(splits[2], (BATCH,), 0, 1000), jax.random.fold_in(splits[2], 1), 0, 999).astype(jnp.int32),
        "skip_grad": centred(splits[3], (BATCH, POS, C), 1.0, 6.0, ((0, 128),)),
        "frozen_one": centred(splits[4], (9 * C, C), (9 * C) ** -0.5, 0.109375, ((0, 16),)),
        "frozen_two": centred(splits[5], (9 * C, C), (9 * C) ** -0.5, 0.109375, ((0, 16),)),
        "time_weight": centred(splits[6], (C, TEMB), C ** -0.5, 0.3125, ((0, 16),)),
        "frozen_emb": centred(splits[7], (TEMB, C), TEMB ** -0.5, 0.15625, ((0, 16),)),
        "train_one": centred(splits[8], (9 * C, C), (9 * C) ** -0.5, 0.109375, ((0, 16),)),
        "train_two": centred(splits[9], (9 * C, C), (9 * C) ** -0.5, 0.109375, ((0, 16),)),
        "train_emb": centred(splits[10], (TEMB, C), TEMB ** -0.5, 0.15625, ((0, 16),)),
        "zero_weight": centred(splits[11], (C, C), C ** -0.5, 0.3125, ((0, 16),)),
    }


group_count = 32
clip_limit = 1.0

def conv_apply(flat, kernel):
    count, chans = flat.shape
    height = count // COLS
    padded = jnp.pad(flat.reshape(height, COLS, chans), ((1, 1), (1, 1), (0, 0)))
    total = jnp.zeros((count, kernel.shape[1]), jnp.float32)
    for offset in range(9):
        row_off = offset // 3
        col_off = offset % 3
        piece = padded[row_off:row_off + height, col_off:col_off + COLS].reshape(count, chans)
        total = total + jnp.dot(piece, kernel[offset * chans:(offset + 1) * chans], preferred_element_type=jnp.float32)
    return total

def conv_back(flat, kernel):
    count, chans = flat.shape
    height = count // COLS
    inner = kernel.shape[0] // 9
    padded = jnp.pad(flat.reshape(height, COLS, chans), ((1, 1), (1, 1), (0, 0)))
    total = jnp.zeros((count, inner), jnp.float32)
    for offset in range(9):
        row_off = offset // 3
        col_off = offset % 3
        piece = padded[2 - row_off:2 - row_off + height, 2 - col_off:2 - col_off + COLS].reshape(count, chans)
        block = kernel[offset * inner:(offset + 1) * inner]
        total = total + lax.dot_general(piece, block, (((1,), (1,)), ((), ())), preferred_element_type=jnp.float32)
    return total

def conv_grads(flat, upstream):
    count, chans = flat.shape
    height = count // COLS
    padded = jnp.pad(flat.reshape(height, COLS, chans), ((1, 1), (1, 1), (0, 0)))
    blocks = []
    for offset in range(9):
        row_off = offset // 3
        col_off = offset % 3
        piece = padded[row_off:row_off + height, col_off:col_off + COLS].reshape(count, chans)
        blocks.append(lax.dot_general(piece, upstream, (((0,), (0,)), ((), ())), preferred_element_type=jnp.float32))
    return jnp.concatenate(blocks, axis=0)

def group_norm(value):
    count, chans = value.shape
    grouped = value.reshape(count, group_count, chans // group_count)
    center = lax.optimization_barrier(jnp.mean(grouped, axis=(0, 2), keepdims=True))
    spread = lax.optimization_barrier(jnp.mean((grouped - center) ** 2, axis=(0, 2), keepdims=True))
    inverse = lax.rsqrt(spread + 1e-05)
    return (((grouped - center) * inverse).reshape(count, chans), inverse)

def norm_back(upstream, normed, inverse):
    count, chans = upstream.shape
    grouped = upstream.reshape(count, group_count, chans // group_count)
    shaped = normed.reshape(count, group_count, chans // group_count)
    first = lax.optimization_barrier(jnp.mean(grouped, axis=(0, 2), keepdims=True))
    second = lax.optimization_barrier(jnp.mean(grouped * shaped, axis=(0, 2), keepdims=True))
    return ((grouped - first - shaped * second) * inverse).reshape(count, chans)

def time_embed(timestep, time_weight):
    half = time_weight.shape[0] // 2
    freqs = jnp.exp(-math.log(10000.0) * jnp.arange(half).astype(jnp.float32) / half)
    angles = timestep.astype(jnp.float32)[:, None] * freqs[None, :]
    wave = jnp.concatenate([jnp.cos(angles), jnp.sin(angles)], axis=1).astype(jnp.bfloat16)
    return jax.nn.silu(jnp.dot(wave, time_weight, preferred_element_type=jnp.float32)).astype(jnp.bfloat16)

def sample_step(latent_one, hint_one, cotangent, emb_one, weights):
    frozen_one, frozen_two, frozen_emb, train_one, train_two, train_emb, zero_weight = weights
    base = latent_one.astype(jnp.float32)
    emb_row = emb_one[None, :]
    fa0 = jax.nn.silu(group_norm(base)[0]).astype(jnp.bfloat16)
    fp1 = conv_apply(fa0, frozen_one) + jnp.dot(emb_row, frozen_emb, preferred_element_type=jnp.float32)
    fa1 = jax.nn.silu(group_norm(fp1)[0]).astype(jnp.bfloat16)
    frozen_out = base + conv_apply(fa1, frozen_two)
    mixed_in = base + hint_one.astype(jnp.float32)
    a_zero = jax.nn.silu(group_norm(mixed_in)[0]).astype(jnp.bfloat16)
    p_one = conv_apply(a_zero, train_one) + jnp.dot(emb_row, train_emb, preferred_element_type=jnp.float32)
    y_one, inverse = group_norm(p_one)
    a_one = jax.nn.silu(y_one).astype(jnp.bfloat16)
    control = (mixed_in + conv_apply(a_one, train_two)).astype(jnp.bfloat16)
    skip_one = (frozen_out + jnp.dot(control, zero_weight, preferred_element_type=jnp.float32)).astype(jnp.bfloat16)
    grad_z = lax.dot_general(control, cotangent, (((0,), (0,)), ((), ())), preferred_element_type=jnp.float32)
    d_control = lax.dot_general(cotangent, zero_weight, (((1,), (1,)), ((), ())), preferred_element_type=jnp.float32).astype(jnp.bfloat16)
    grad_w2 = conv_grads(a_one, d_control)
    d_aone = conv_back(d_control, train_two)
    sig = jax.nn.sigmoid(y_one)
    d_yone = d_aone * sig * (1.0 + y_one * (1.0 - sig))
    d_pone = norm_back(d_yone, y_one, inverse)
    grad_e = emb_one.astype(jnp.float32)[:, None] * lax.optimization_barrier(jnp.sum(d_pone, axis=0))[None, :]
    grad_w1 = conv_grads(a_zero, d_pone.astype(jnp.bfloat16))
    return (skip_one, (grad_w1, grad_w2, grad_e, grad_z))

def run_batch(latent, hint, skip_grad, emb, weights):
    train_one, train_emb, zero_weight = (weights[3], weights[5], weights[6])
    start = (jnp.zeros(train_one.shape, jnp.float32), jnp.zeros(train_one.shape, jnp.float32), jnp.zeros(train_emb.shape, jnp.float32), jnp.zeros(zero_weight.shape, jnp.float32))

    def advance(carry, items):
        skip_one, grads = sample_step(items[0], items[1], items[2], items[3], weights)
        return (tuple((old + new for old, new in zip(carry, grads))), skip_one)
    grads, skips = lax.scan(advance, start, (latent, hint, skip_grad, emb))
    return (skips, grads)

def reference(latent, hint, timestep, skip_grad, frozen_one, frozen_two, time_weight, frozen_emb, train_one, train_two, train_emb, zero_weight):
    emb = time_embed(timestep, time_weight)
    weights = (frozen_one, frozen_two, frozen_emb, train_one, train_two, train_emb, zero_weight)
    skips, grads = run_batch(latent, hint, skip_grad, emb, weights)
    total = sum((jnp.sum(item * item) for item in grads))
    grad_norm = jnp.sqrt(total + 1e-06)
    scale = jnp.minimum(1.0, clip_limit / grad_norm)
    return (skips, grads[0] * scale, grads[1] * scale, grads[2] * scale, grads[3] * scale, grad_norm)
```

```python
import math

import jax
import jax.numpy as jnp
from jax import lax
from jax.experimental import pallas as pl
from jax.experimental.pallas import tpu as pltpu
from jax.sharding import PartitionSpec as P

COLS = 64


clip_limit = 1.0


def sent_together(arrays, axis, dim, along):
    both = jnp.concatenate(arrays, axis=along)
    out, at, gathered = (lax.all_gather(both, axis, axis=dim, tiled=True), 0, [])
    for a in arrays:
        gathered.append(lax.slice_in_dim(out, at, at + a.shape[along], axis=along))
        at += a.shape[along]
    return tuple(gathered)


def laid_out(tiles, dim):
    tiles = jnp.moveaxis(tiles, 0, dim)
    shape = tiles.shape
    return tiles.reshape(*shape[:dim], shape[dim] * shape[dim + 1], *shape[dim + 2 :])


def gather_packed(arrays, axis, dims):
    vector = jnp.concatenate([a.reshape(-1) for a in arrays])
    lines, at, gathered = (lax.all_gather(vector, axis), 0, [])
    for a, dim in zip(arrays, dims):
        tiles = lines[:, at : at + a.size].reshape(-1, *a.shape)
        gathered.append(laid_out(tiles, dim))
        at += a.size
    return tuple(gathered)


def cut_along(value, dim, size):
    before, after = (value.shape[:dim], value.shape[dim + 1 :])
    return jnp.moveaxis(value.reshape(*before, size, -1, *after), dim, 0)


def sum_packed(arrays, axis, dims):
    size = lax.axis_size(axis)
    tiles = [cut_along(a, dim, size) for a, dim in zip(arrays, dims)]
    lines = jnp.concatenate([b.reshape(size, -1) for b in tiles], axis=1)
    span = max(16, -(-lines.shape[1] // 1024) * 8)
    lines = jnp.pad(lines, ((0, 0), (0, span * 128 - lines.shape[1]))).reshape(-1, 128)
    vector, at, gathered = (lax.psum_scatter(lines, axis, tiled=True).reshape(-1), 0, [])
    for b in tiles:
        part = b[0]
        gathered.append(vector[at : at + part.size].reshape(part.shape))
        at += part.size
    return tuple(gathered)


def sent_to_all(value, axis):
    copies = jnp.broadcast_to(value, (lax.axis_size(axis), *value.shape))
    return lax.all_to_all(copies, axis, split_axis=0, concat_axis=0, tiled=True)


def taken_together(value, axis):
    return sent_to_all(value, axis).astype(jnp.float32).sum(axis=0)


def of_everyone(value, axis):
    everything = sent_to_all(value, axis)
    return jnp.sum(everything, axis=0)


POS = 1024
C = 320
TILE = 128
STEPS = POS // TILE
MT = 256
F32 = jnp.float32
BF = jnp.bfloat16
EPS = 1e-05
COUNT = POS * 10.0


def rows(i, size, base=0):
    return pl.ds(pl.multiple_of(i * size + base, 16), size)


def group_matrix():
    r = lax.broadcasted_iota(jnp.int32, (C, C), 0)
    c = lax.broadcasted_iota(jnp.int32, (C, C), 1)
    return ((r * 6554) // 65536 == (c * 6554) // 65536).astype(F32)


def fold(x):
    return x.reshape(TILE // 8, 8, C).sum(axis=0)


def group_mean(part, g_ref):
    total = jnp.dot(part, g_ref[...], preferred_element_type=F32, precision=lax.Precision.HIGHEST)
    return jnp.sum(total, axis=0, keepdims=True) * (1.0 / COUNT)


def stats(read, g_ref):
    zero = jnp.zeros((8, C), F32)
    mean = group_mean(lax.fori_loop(0, STEPS, lambda i, s: s + fold(read(i)), zero), g_ref)

    def square(i, s):
        d = read(i) - mean
        return s + fold(d * d)

    var = group_mean(lax.fori_loop(0, STEPS, square, zero), g_ref)
    return mean, lax.rsqrt(var + EPS)


def put_shifted(x, ref, i, order):
    j = lax.broadcasted_iota(jnp.int32, (TILE, C), 0) % COLS
    before = jnp.where(j == 0, 0.0, pltpu.roll(x, 1, 0)).astype(BF)
    after = jnp.where(j == COLS - 1, 0.0, pltpu.roll(x, TILE - 1, 0)).astype(BF)
    mid = x.astype(BF)
    parts = (before, mid, after) if order > 0 else (after, mid, before)
    ref[rows(i, TILE, COLS), :] = jnp.concatenate(parts, axis=1)


def clear_edges(ref):
    z = jnp.zeros((COLS, ref.shape[1]), ref.dtype)
    ref[0:COLS, :] = z
    ref[COLS + POS : 2 * COLS + POS, :] = z


def normed_silu(read, x3, g_ref):
    mean, inverse = stats(read, g_ref)

    def body(i, c):
        y = (read(i) - mean) * inverse
        put_shifted(y * jax.nn.sigmoid(y), x3, i, 1)
        return c

    lax.fori_loop(0, STEPS, body, 0)


def conv(x3, w_ref, write):
    def body(m, c):
        acc = None
        for a in range(3):
            t = jnp.dot(
                x3[rows(m, MT, a * COLS), :], w_ref[a * 960 : (a + 1) * 960, :], preferred_element_type=F32
            )
            acc = t if acc is None else acc + t
        write(m, acc)
        return c

    lax.fori_loop(0, POS // MT, body, 0)


def conv_back(d3, w_ref, write):
    def body(m, c):
        acc = None
        for a in range(3):
            for b in range(3):
                k = 3 * a + b
                t = lax.dot_general(
                    d3[rows(m, MT, (2 - a) * COLS), b * C : (b + 1) * C],
                    w_ref[k * C : (k + 1) * C, :],
                    (((1,), (1,)), ((), ())),
                    preferred_element_type=F32,
                )
                acc = t if acc is None else acc + t
        write(m, acc)
        return c

    lax.fori_loop(0, POS // MT, body, 0)


def conv_grads(x3, dp, out):
    for b in range(3):
        lhs = x3[COLS : COLS + POS, b * C : (b + 1) * C]
        for a in range(3):
            k = 3 * a + b
            t = lax.dot_general(
                lhs, dp[128 - 64 * a : 128 - 64 * a + POS, :], (((0,), (0,)), ((), ())), preferred_element_type=F32
            )
            out[k * C : (k + 1) * C, :] = t.astype(BF)


def kernel(
    lat, hint, sg, ef, et, f1, f2, t1, t2, zw,
    skip, dw1, dw2, dz, esum,
    g_ref, xa, xb, d3, dp, y1, p, ctl,
):
    g_ref[...] = group_matrix()
    for r in (xa, xb, d3, dp):
        clear_edges(r)

    def latent_at(i):
        return lat[rows(i, TILE), :].astype(F32)

    def mixed_at(i):
        return latent_at(i) + hint[rows(i, TILE), :].astype(F32)

    def p_at(i):
        return p[rows(i, TILE), :]

    normed_silu(mixed_at, xa, g_ref)

    def dc_body(i, c):
        d = lax.dot_general(sg[rows(i, TILE), :], zw[...], (((1,), (1,)), ((), ())), preferred_element_type=F32)
        d = d.astype(BF).astype(F32)
        dp[rows(i, TILE, COLS), :] = d.astype(BF)
        put_shifted(d, d3, i, -1)
        return c

    lax.fori_loop(0, STEPS, dc_body, 0)

    def put_p(e):
        def write(m, acc):
            p[rows(m, MT), :] = acc + e
        return write

    conv(xa, t1, put_p(et[...]))
    mean, inverse = stats(p_at, g_ref)

    def y_body(i, c):
        y = (p_at(i) - mean) * inverse
        y1[rows(i, TILE), :] = y
        put_shifted(y * jax.nn.sigmoid(y), xb, i, 1)
        return c

    lax.fori_loop(0, STEPS, y_body, 0)
    conv_grads(xb, dp, dw2)

    def write_da(m, acc):
        p[rows(m, MT), :] = acc

    conv_back(d3, t2, write_da)
    zero = jnp.zeros((8, C), F32)

    def dy_body(i, s):
        y = y1[rows(i, TILE), :]
        sig = jax.nn.sigmoid(y)
        dy = p_at(i) * sig * (1.0 + y * (1.0 - sig))
        p[rows(i, TILE), :] = dy
        return s[0] + fold(dy), s[1] + fold(dy * y)

    s1, s2 = lax.fori_loop(0, STEPS, dy_body, (zero, zero))
    m1, m2 = group_mean(s1, g_ref), group_mean(s2, g_ref)

    def dp_body(i, s):
        d = (p_at(i) - m1 - y1[rows(i, TILE), :] * m2) * inverse
        dp[rows(i, TILE, COLS), :] = d.astype(BF)
        return s + fold(d)

    esum[...] = jnp.sum(lax.fori_loop(0, STEPS, dp_body, zero), axis=0, keepdims=True)
    conv_grads(xa, dp, dw1)

    def write_control(m, acc):
        mixed = lat[rows(m, MT), :].astype(F32) + hint[rows(m, MT), :].astype(F32)
        ctl[rows(m, MT), :] = (mixed + acc).astype(BF)

    conv(xb, t2, write_control)
    dz[...] = lax.dot_general(ctl[...], sg[...], (((0,), (0,)), ((), ())), preferred_element_type=F32).astype(BF)

    normed_silu(latent_at, xa, g_ref)
    conv(xa, f1, put_p(ef[...]))
    normed_silu(p_at, xb, g_ref)

    def write_skip(m, acc):
        out = lat[rows(m, MT), :].astype(F32) + acc
        out = out + jnp.dot(ctl[rows(m, MT), :], zw[...], preferred_element_type=F32)
        skip[rows(m, MT), :] = out.astype(BF)

    conv(xb, f2, write_skip)


SCRATCH = [
    pltpu.VMEM((C, C), F32),
    pltpu.VMEM((POS + 2 * COLS, 3 * C), BF),
    pltpu.VMEM((POS + 2 * COLS, 3 * C), BF),
    pltpu.VMEM((POS + 2 * COLS, 3 * C), BF),
    pltpu.VMEM((POS + 2 * COLS, C), BF),
    pltpu.VMEM((POS, C), F32),
    pltpu.VMEM((POS, C), F32),
    pltpu.VMEM((POS, C), BF),
]


def compute(lat, hint, sg, ef, et, f1, f2, t1, t2, zw):
    vm = pl.BlockSpec(memory_space=pltpu.VMEM)
    return pl.pallas_call(
        kernel,
        out_shape=(
            jax.ShapeDtypeStruct((POS, C), BF),
            jax.ShapeDtypeStruct((9 * C, C), BF),
            jax.ShapeDtypeStruct((9 * C, C), BF),
            jax.ShapeDtypeStruct((C, C), BF),
            jax.ShapeDtypeStruct((1, C), F32),
        ),
        in_specs=[vm] * 10,
        out_specs=[vm] * 5,
        scratch_shapes=SCRATCH,
        compiler_params=pltpu.CompilerParams(vmem_limit_bytes=64000000),
    )(lat, hint, sg, ef, et, f1, f2, t1, t2, zw)


def time_embed(timestep, time_weight):
    half = time_weight.shape[0] // 2
    freqs = jnp.exp(-math.log(10000.0) * jnp.arange(half).astype(jnp.float32) / half)
    angles = timestep.astype(jnp.float32)[:, None] * freqs[None, :]
    wave = jnp.concatenate([jnp.cos(angles), jnp.sin(angles)], axis=1).astype(jnp.bfloat16)
    return jax.nn.silu(jnp.dot(wave, time_weight, preferred_element_type=jnp.float32)).astype(
        jnp.bfloat16
    )


def shards(
    latent,
    hint,
    timestep,
    skip_grad,
    frozen_one,
    frozen_two,
    time_weight,
    frozen_emb,
    train_one,
    train_two,
    train_emb,
    zero_weight,
):
    frozen_full = (
        *sent_together((frozen_one, frozen_two), "fsdp", 0, 1),
        lax.all_gather(time_weight, "fsdp", axis=0, tiled=True),
        lax.all_gather(frozen_emb, "fsdp", axis=0, tiled=True),
    )
    train_full = gather_packed((train_one, train_two, train_emb, zero_weight), "fsdp", (0, 0, 0, 0))
    emb = time_embed(timestep, frozen_full[2])
    frozen_row = jnp.dot(emb, frozen_full[3], preferred_element_type=F32)
    train_row = jnp.dot(emb, train_full[2], preferred_element_type=F32)
    skip, dw1, dw2, dz, esum = compute(
        latent[0], hint[0], skip_grad[0], frozen_row, train_row,
        frozen_full[0], frozen_full[1], train_full[0], train_full[1], train_full[3],
    )
    skips = skip[None]
    grads = (dw1, dw2, emb[0].astype(F32)[:, None] * esum, dz)
    partial_rows = tuple(
        (
            part.astype(jnp.float32)
            for part in sum_packed(
                (
                    grads[0].astype(jnp.bfloat16),
                    grads[1].astype(jnp.bfloat16),
                    grads[2].astype(jnp.bfloat16),
                    grads[3].astype(jnp.bfloat16),
                ),
                "fsdp",
                (0, 0, 0, 0),
            )
        )
    )
    owned = (
        taken_together(partial_rows[0].astype(jnp.bfloat16), "dp").astype(jnp.float32),
        taken_together(partial_rows[1].astype(jnp.bfloat16), "dp").astype(jnp.float32),
        taken_together(partial_rows[2].astype(jnp.bfloat16), "dp").astype(jnp.float32),
        taken_together(partial_rows[3].astype(jnp.bfloat16), "dp").astype(jnp.float32),
    )
    local_sum = sum((jnp.sum(item * item) for item in owned))
    total = of_everyone(local_sum, "fsdp")
    grad_norm = jnp.sqrt(total + 1e-06)
    scale = jnp.minimum(1.0, clip_limit / grad_norm)
    return (
        skips,
        owned[0] * scale,
        owned[1] * scale,
        owned[2] * scale,
        owned[3] * scale,
        grad_norm,
    )


def solution(mesh):
    in_specs = (
        P(("dp", "fsdp"), None, None),
        P(("dp", "fsdp"), None, None),
        P(("dp", "fsdp")),
        P(("dp", "fsdp"), None, None),
        P("fsdp", None),
        P("fsdp", None),
        P("fsdp", None),
        P("fsdp", None),
        P("fsdp", None),
        P("fsdp", None),
        P("fsdp", None),
        P("fsdp", None),
    )
    out_specs = (
        P(("dp", "fsdp"), None, None),
        P("fsdp", None),
        P("fsdp", None),
        P("fsdp", None),
        P("fsdp", None),
        P(),
    )
    return jax.shard_map(shards, mesh=mesh, in_specs=in_specs, out_specs=out_specs, check_vma=False)
```

```python
import math

import jax
import jax.numpy as jnp
from jax import lax
from jax.experimental import pallas as pl
from jax.experimental.pallas import tpu as pltpu
from jax.sharding import PartitionSpec as P

COLS = 64
POS = 1024
C = 320
TEMB = 1280
TILE = 128
STEPS = POS // TILE
MT = 256
HALF = 90
HALF_Z = 100
CUT = 48
F32 = jnp.float32
BF = jnp.bfloat16
EPS = 1e-05
COUNT = POS * 10.0
clip_limit = 1.0
EXACT = lax.Precision.HIGHEST
MESH = pl.DeviceIdType.MESH


def rows(i, size, base=0):
    return pl.ds(pl.multiple_of(i * size + base, 16), size)


def group_matrix():
    r = lax.broadcasted_iota(jnp.int32, (C, C), 0)
    c = lax.broadcasted_iota(jnp.int32, (C, C), 1)
    return ((r * 6554) // 65536 == (c * 6554) // 65536).astype(F32)


def fold(x):
    return x.reshape(TILE // 8, 8, C).sum(axis=0)


def group_mean(part, g_ref):
    total = jnp.dot(part, g_ref[...], preferred_element_type=F32, precision=lax.Precision.HIGHEST)
    return jnp.sum(total, axis=0, keepdims=True) * (1.0 / COUNT)


def stats(read, g_ref):
    zero = jnp.zeros((8, C), F32)
    mean = group_mean(lax.fori_loop(0, STEPS, lambda i, s: s + fold(read(i)), zero), g_ref)

    def square(i, s):
        d = read(i) - mean
        return s + fold(d * d)

    var = group_mean(lax.fori_loop(0, STEPS, square, zero), g_ref)
    return mean, lax.rsqrt(var + EPS)


def put_shifted(x, ref, i, order):
    j = lax.broadcasted_iota(jnp.int32, (TILE, C), 0) % COLS
    before = jnp.where(j == 0, 0.0, pltpu.roll(x, 1, 0)).astype(BF)
    after = jnp.where(j == COLS - 1, 0.0, pltpu.roll(x, TILE - 1, 0)).astype(BF)
    mid = x.astype(BF)
    parts = (before, mid, after) if order > 0 else (after, mid, before)
    ref[rows(i, TILE, COLS), :] = jnp.concatenate(parts, axis=1)


def clear_edges(ref):
    z = jnp.zeros((COLS, ref.shape[1]), ref.dtype)
    ref[0:COLS, :] = z
    ref[COLS + POS : 2 * COLS + POS, :] = z


def normed_silu(read, x3, g_ref):
    mean, inverse = stats(read, g_ref)

    def body(i, c):
        y = (read(i) - mean) * inverse
        put_shifted(y * jax.nn.sigmoid(y), x3, i, 1)
        return c

    lax.fori_loop(0, STEPS, body, 0)


def conv(x3, w_ref, write):
    def body(m, c):
        acc = None
        for a in range(3):
            t = jnp.dot(
                x3[rows(m, MT, a * COLS), :], w_ref[a * 960 : (a + 1) * 960, :], preferred_element_type=F32
            )
            acc = t if acc is None else acc + t
        write(m, acc)
        return c

    lax.fori_loop(0, POS // MT, body, 0)


def conv_back(d3, w_ref, write):
    def body(m, c):
        acc = None
        for a in range(3):
            for b in range(3):
                k = 3 * a + b
                t = lax.dot_general(
                    d3[rows(m, MT, (2 - a) * COLS), b * C : (b + 1) * C],
                    w_ref[k * C : (k + 1) * C, :],
                    (((1,), (1,)), ((), ())),
                    preferred_element_type=F32,
                )
                acc = t if acc is None else acc + t
        write(m, acc)
        return c

    lax.fori_loop(0, POS // MT, body, 0)


def turned(src, dst):
    def body(i, c):
        cols = pl.ds(pl.multiple_of(i * TILE, TILE), TILE)
        dst[rows(i, TILE), :] = src[:, cols].astype(F32).T.astype(BF)
        return c

    lax.fori_loop(0, STEPS, body, 0)


def paired(ref, dst, at, size):
    dst[at : at + size, 0:C] = ref[0:size, :]
    dst[at : at + size, C : 2 * C] = ref[size : 2 * size, :]


def add_into(dst, *others):
    total = dst[...].astype(F32)
    for o in others:
        total = total + o[...].astype(F32)
    dst[...] = total.astype(BF)


def kernel(
    lat_t, hint_t, sg_t, wave, f1, f2, tw, fe, t1, t2, te, zw,
    skip, o1, o2, oe, oz, onorm,
    lat, hint, sg, g_ref, xa, xb, xf, d3, dp, y1, p, ctl, dw,
    w1, w2, v1, v2, wz,
    ga, gb, gc, gd,
    wv, pb, pr, rb, rr, em, es, nr,
    out_a, out_b, in_a, in_b, xp_a, xp_b, xq_a, xq_b, zb_a, zb_b, cur_a, cur_b, got_a, got_b,
    g_send, g_recv, e_send, e_recv, r_send, r_recv,
):
    me_dp, me = lax.axis_index("dp"), lax.axis_index("fsdp")
    core, zh, x = lax.rem(me, 2), lax.rem(me // 2, 2), me // 4
    y, zl = me_dp // 2, lax.rem(me_dp, 2)
    oc, oh, ol = 1 - core, 1 - zh, 1 - zl
    xr, xl, xo = lax.rem(x + 1, 4), lax.rem(x + 3, 4), lax.rem(x + 2, 4)
    y_near = y + 1 - 2 * lax.rem(y, 2)
    right = (me_dp, xr * 4 + zh * 2 + core)
    left = (me_dp, xl * 4 + zh * 2 + core)
    mate = (me_dp, x * 4 + zh * 2 + oc)
    z_b = (y * 2 + ol, x * 4 + oh * 2 + core)
    z_a = (y * 2 + ol, me)
    y_a = (y_near * 2 + zl, me)
    y_b = ((3 - y) * 2 + zl, me)

    started = []

    def send(src, dst, ssem, rsem, to):
        c = pltpu.make_async_remote_copy(
            src_ref=src, dst_ref=dst, send_sem=ssem, recv_sem=rsem, device_id=to, device_id_type=MESH
        )
        c.start()
        started.append(c)

    def landed(ref, rsem):
        pltpu.make_async_remote_copy(
            src_ref=ref, dst_ref=ref, send_sem=rsem, recv_sem=rsem, device_id=mate, device_id_type=MESH
        ).wait_recv()

    gathered = (ga, gb, gc, gd)
    own = x * 2 + zh
    paired(t1, ga.at[core, own], 0, HALF)
    paired(zw, ga.at[core, own], HALF, 10)
    barrier = pltpu.get_barrier_semaphore()

    def greet(k, c):
        pl.semaphore_signal(barrier, inc=1, device_id=(me_dp, lax.rem(me + k, 16)), device_id_type=MESH)
        return c

    lax.fori_loop(1, 16, greet, 0)
    for to in (z_b, z_a, y_a, y_b):
        pl.semaphore_signal(barrier, inc=1, device_id=to, device_id_type=MESH)
    paired(t2, gb.at[core, own], 0, HALF)
    paired(f1, gc.at[core, own], 0, HALF)
    paired(f2, gd.at[core, own], 0, HALF)
    wv[me] = wave[...]
    pl.semaphore_wait(barrier, 19)

    def block(w, j):
        return gathered[w].at[core, j]

    def pass_on(w, j, n):
        send(block(w, j), block(w, j), g_send.at[w, n], g_recv.at[w, 8 + n], mate)

    def low(w, j):
        return gathered[w].at[core, j, pl.ds(0, CUT)]

    def high(w, j):
        return gathered[w].at[core, j, pl.ds(CUT, gathered[w].shape[2] - CUT)]

    def g1(w):
        b = block(w, own)
        send(b, b, g_send.at[w, 8], g_recv.at[w, 0], right)
        send(b, b, g_send.at[w, 9], g_recv.at[w, 1], left)
        send(b, b, g_send.at[w, 10], g_recv.at[w, 2], z_b)
        pass_on(w, own, 0)

    def g2(w):
        jl, jr, jz = xl * 2 + zh, xr * 2 + zh, x * 2 + oh
        landed(block(w, jl), g_recv.at[w, 0])
        send(low(w, jl), low(w, jl), g_send.at[w, 11], g_recv.at[w, 3], right)
        landed(block(w, jr), g_recv.at[w, 1])
        send(high(w, jr), high(w, jr), g_send.at[w, 12], g_recv.at[w, 4], left)
        landed(block(w, jz), g_recv.at[w, 2])
        send(block(w, jz), block(w, jz), g_send.at[w, 13], g_recv.at[w, 5], right)
        send(block(w, jz), block(w, jz), g_send.at[w, 14], g_recv.at[w, 6], left)
        pass_on(w, jl, 1)
        pass_on(w, jr, 2)
        pass_on(w, jz, 3)

    def g3(w):
        jo, jl, jr = xo * 2 + zh, xl * 2 + oh, xr * 2 + oh
        landed(low(w, jo), g_recv.at[w, 3])
        landed(high(w, jo), g_recv.at[w, 4])
        send(block(w, jo), block(w, jo), g_send.at[w, 15], g_recv.at[w, 7], z_b)
        pass_on(w, jo, 4)
        landed(block(w, jl), g_recv.at[w, 5])
        pass_on(w, jl, 5)
        landed(block(w, jr), g_recv.at[w, 6])
        pass_on(w, jr, 6)

    def g4(w):
        jz = xo * 2 + oh
        landed(block(w, jz), g_recv.at[w, 7])
        pass_on(w, jz, 7)

    def g5(w, full):
        order = (
            x * 2 + zh, xl * 2 + zh, xr * 2 + zh, x * 2 + oh, xo * 2 + zh, xl * 2 + oh, xr * 2 + oh, xo * 2 + oh
        )
        for n, j in enumerate(order):
            landed(gathered[w].at[oc, j], g_recv.at[w, 8 + n])
        g = gathered[w]
        for d in range(16):
            for h in range(2):
                full[d * 180 + h * HALF : d * 180 + (h + 1) * HALF, :] = g[
                    d % 2, d // 2, 0:HALF, h * C : (h + 1) * C
                ]

    def spread(n, src_of, dst):
        def body(k, c):
            to = lax.rem(me + k, 16)
            pltpu.make_async_remote_copy(
                src_ref=src_of(to), dst_ref=dst.at[me], send_sem=e_send.at[n, to], recv_sem=e_recv.at[n, me],
                device_id=(me_dp, to), device_id_type=MESH,
            ).start()
            return c

        lax.fori_loop(1, 16, body, 0)

    def spread_wait(n, dst):
        def body(k, c):
            slot = lax.rem(me + k, 16)
            pltpu.make_async_remote_copy(
                src_ref=dst.at[slot], dst_ref=dst.at[slot], send_sem=e_send.at[n, slot], recv_sem=e_recv.at[n, slot],
                device_id=(me_dp, slot), device_id_type=MESH,
            ).wait_recv()
            return c

        lax.fori_loop(1, 16, body, 0)

    def spread_sent(n, src_of, dst):
        def body(k, c):
            to = lax.rem(me + k, 16)
            pltpu.make_async_remote_copy(
                src_ref=src_of(to), dst_ref=dst.at[me], send_sem=e_send.at[n, to], recv_sem=e_recv.at[n, me],
                device_id=(me_dp, to), device_id_type=MESH,
            ).wait_send()
            return c

        lax.fori_loop(1, 16, body, 0)

    def stacked(ref):
        return jnp.concatenate([ref[s] for s in range(16)], axis=0)

    g1(0)
    spread(0, lambda to: wv.at[me], wv)
    g1(1)
    g_ref[...] = group_matrix()
    for r in (xa, xb, xf, d3, dp):
        clear_edges(r)
    turned(lat_t, lat)
    turned(hint_t, hint)

    def latent_at(i):
        return lat[rows(i, TILE), :].astype(F32)

    def mixed_at(i):
        return latent_at(i) + hint[rows(i, TILE), :].astype(F32)

    def p_at(i):
        return p[rows(i, TILE), :]

    g2(0)
    spread_wait(0, wv)
    pick = lax.broadcasted_iota(jnp.int32, (C, 20), 0) == me * 20 + lax.broadcasted_iota(jnp.int32, (C, 20), 1)
    mine = jnp.dot(stacked(wv).astype(BF), pick.astype(F32).astype(BF), preferred_element_type=F32).astype(BF)
    pre = jnp.dot(mine, tw[...], preferred_element_type=F32)
    for e in range(16):
        pb[e] = pre[:, e * 80 : (e + 1) * 80]
    pr[me] = pb[me]
    spread(1, lambda to: pb.at[to], pr)
    turned(sg_t, sg)
    normed_silu(mixed_at, xa, g_ref)
    g3(0)
    g2(1)
    g1(2)
    spread_wait(1, pr)
    total = pr[0]
    for s in range(1, 16):
        total = total + pr[s]
    em[...] = (total * jax.nn.sigmoid(total)).astype(BF).astype(F32)
    emb = em[...].astype(BF)
    row_f = jnp.dot(emb, fe[...], preferred_element_type=F32)
    row_t = jnp.dot(emb, te[...], preferred_element_type=F32)
    both = jnp.concatenate([row_f, row_t], axis=1)
    for s in range(16):
        rb[s] = both[s : s + 1, :]
    rr[me] = rb[me]
    spread(2, lambda to: rb.at[to], rr)
    g4(0)
    normed_silu(latent_at, xf, g_ref)
    g3(1)
    g2(2)
    g1(3)
    spread_wait(2, rr)
    row = rr[0]
    for s in range(1, 16):
        row = row + rr[s]
    frozen_row, train_row = row[:, 0:C], row[:, C : 2 * C]
    g5(0, w1)
    for d in range(16):
        for h in range(2):
            wz[d * 20 + h * 10 : d * 20 + (h + 1) * 10, :] = ga[d % 2, d // 2, HALF:HALF_Z, h * C : (h + 1) * C]

    def put_p(e):
        def write(m, acc):
            p[rows(m, MT), :] = acc + e

        return write

    conv(xa, w1, put_p(train_row))
    g4(1)
    g3(2)
    g2(3)

    def dc_body(i, c):
        d = lax.dot_general(sg[rows(i, TILE), :], wz[...], (((1,), (1,)), ((), ())), preferred_element_type=F32)
        d = d.astype(BF).astype(F32)
        dp[rows(i, TILE, COLS), :] = d.astype(BF)
        put_shifted(d, d3, i, -1)
        return c

    lax.fori_loop(0, STEPS, dc_body, 0)
    mean, inverse = stats(p_at, g_ref)

    def y_body(i, c):
        v = (p_at(i) - mean) * inverse
        y1[rows(i, TILE), :] = v
        put_shifted(v * jax.nn.sigmoid(v), xb, i, 1)
        return c

    lax.fori_loop(0, STEPS, y_body, 0)
    g5(1, w2)
    g4(2)
    g3(3)

    def write_control(m, acc):
        mixed = lat[rows(m, MT), :].astype(F32) + hint[rows(m, MT), :].astype(F32)
        ctl[rows(m, MT), :] = (mixed + acc).astype(BF)

    conv(xb, w2, write_control)
    g4(3)

    sums = (
        (out_a, in_a, xp_a, xq_a, zb_a, cur_a, got_a),
        (out_b, in_b, xp_b, xq_b, zb_b, cur_b, got_b),
    )

    def packed(n):
        out = sums[n][0]
        for d in range(16):
            for h in range(2):
                out[d % 2, d // 2, 0:HALF, h * C : (h + 1) * C] = dw[
                    d * 180 + h * HALF : d * 180 + (h + 1) * HALF, :
                ]

    def r1(n):
        out, inn = sums[n][:2]
        send(out.at[oc], inn, r_send.at[n, 0], r_recv.at[n, 0], mate)

    def r2(n):
        out, inn, xp = sums[n][:3]
        landed(inn, r_recv.at[n, 0])
        for h in range(2):
            j = xo * 2 + h
            add_into(out.at[core, j], inn.at[j])
            send(out.at[core, j], xp.at[h], r_send.at[n, 1 + h], r_recv.at[n, 1 + h], (right, left)[h])
        for xs in (xr, xl, x):
            for h in range(2):
                add_into(out.at[core, xs * 2 + h], inn.at[xs * 2 + h])

    def r3(n):
        out, _, xp, xq = sums[n][:4]
        for h in range(2):
            landed(xp.at[h], r_recv.at[n, 1 + h])
            xs = (xr, xl)[h]
            add_into(out.at[core, xs * 2 + h], xp.at[h])
            send(out.at[core, pl.ds(xs * 2, 2)], xq.at[h], r_send.at[n, 3 + h], r_recv.at[n, 3 + h], (right, left)[h])

    def r4(n):
        out, _, _, xq, zb = sums[n][:5]
        landed(xq.at[0], r_recv.at[n, 3])
        landed(xq.at[1], r_recv.at[n, 4])
        add_into(out.at[core, x * 2 + oh], xq.at[0, oh], xq.at[1, oh])
        send(out.at[core, x * 2 + oh], zb, r_send.at[n, 5], r_recv.at[n, 5], z_b)
        add_into(out.at[core, x * 2 + zh], xq.at[0, zh], xq.at[1, zh])

    def r5(n):
        out, _, _, _, zb, cur, got = sums[n]
        size = zb.shape[0]
        landed(zb, r_recv.at[n, 5])
        cur[0, 0:size, :] = (out[core, x * 2 + zh].astype(F32) + zb[...].astype(F32)).astype(BF)
        send(cur.at[0], got.at[0], r_send.at[n, 6], r_recv.at[n, 6], z_a)

    def r6(n, k):
        cur, got = sums[n][5:7]
        landed(got.at[k], r_recv.at[n, 6 + k])
        cur[k + 1] = (cur[k].astype(F32) + got[k].astype(F32)).astype(BF)
        send(cur.at[k + 1], got.at[k + 1], r_send.at[n, 7 + k], r_recv.at[n, 7 + k], (y_a, y_b)[k])

    def conv_grad_dots(x3):
        for b in range(3):
            lhs = x3[COLS : COLS + POS, b * C : (b + 1) * C]
            for a in range(3):
                k = 3 * a + b
                t = lax.dot_general(
                    lhs, dp[128 - 64 * a : 128 - 64 * a + POS, :], (((0,), (0,)), ((), ())),
                    preferred_element_type=F32,
                )
                dw[k * C : (k + 1) * C, :] = t.astype(BF)

    dz = lax.dot_general(ctl[...], sg[...], (((0,), (0,)), ((), ())), preferred_element_type=F32)
    for d in range(16):
        for h in range(2):
            at = d * 20 + h * 10
            out_a[d % 2, d // 2, HALF:HALF_Z, h * C : (h + 1) * C] = dz[at : at + 10, :].astype(BF)
    conv_grad_dots(xb)
    packed(0)
    r1(0)
    g5(2, v1)

    def write_da(m, acc):
        p[rows(m, MT), :] = acc

    conv_back(d3, w2, write_da)
    r2(0)
    zero = jnp.zeros((8, C), F32)

    def dy_body(i, s):
        v = y1[rows(i, TILE), :]
        sig = jax.nn.sigmoid(v)
        dy = p_at(i) * sig * (1.0 + v * (1.0 - sig))
        p[rows(i, TILE), :] = dy
        return s[0] + fold(dy), s[1] + fold(dy * v)

    s1, s2 = lax.fori_loop(0, STEPS, dy_body, (zero, zero))
    m1, m2 = group_mean(s1, g_ref), group_mean(s2, g_ref)

    def dp_body(i, s):
        d = (p_at(i) - m1 - y1[rows(i, TILE), :] * m2) * inverse
        dp[rows(i, TILE, COLS), :] = d.astype(BF)
        return s + fold(d)

    es[me] = jnp.sum(lax.fori_loop(0, STEPS, dp_body, zero), axis=0, keepdims=True)
    spread(3, lambda to: es.at[me], es)
    r3(0)
    conv_grad_dots(xa)
    packed(1)
    r1(1)
    r4(0)
    g5(3, v2)
    conv(xf, v1, put_p(frozen_row))
    r2(1)
    r5(0)
    spread_wait(3, es)
    de = lax.dot_general(
        em[...], stacked(es), (((0,), (0,)), ((), ())), preferred_element_type=F32, precision=EXACT
    )
    for h in range(2):
        cur_b[0, HALF : HALF + 40, h * C : (h + 1) * C] = de[h * 40 : (h + 1) * 40, :].astype(BF)
    normed_silu(p_at, xf, g_ref)
    r3(1)
    r6(0, 0)

    def write_skip(m, acc):
        out = lat[rows(m, MT), :].astype(F32) + acc
        out = out + jnp.dot(ctl[rows(m, MT), :], wz[...], preferred_element_type=F32)
        skip[:, pl.ds(pl.multiple_of(m * MT, MT), MT)] = out.T.astype(BF)

    conv(xf, v2, write_skip)
    r4(1)
    r6(0, 1)
    r5(1)
    r6(1, 0)
    r6(1, 1)
    landed(got_a.at[2], r_recv.at[0, 8])
    tot_a = cur_a[2].astype(F32) + got_a[2].astype(F32)
    sq = jnp.sum(tot_a * tot_a, axis=0, keepdims=True)
    landed(got_b.at[2], r_recv.at[1, 8])
    tot_b = cur_b[2].astype(F32) + got_b[2].astype(F32)
    sq = sq + jnp.sum(tot_b * tot_b, axis=0, keepdims=True)
    nr[me] = jnp.broadcast_to(jnp.sum(sq, axis=1, keepdims=True), (1, 128))
    spread(4, lambda to: nr.at[me], nr)
    spread_wait(4, nr)
    total = nr[0]
    for s in range(1, 16):
        total = total + nr[s]
    norm = jnp.sqrt(total[:, 0:1] + 1e-06)
    scale = jnp.minimum(1.0, clip_limit / norm)
    onorm[...] = norm
    for h in range(2):
        c = slice(h * C, (h + 1) * C)
        o2[h * HALF : (h + 1) * HALF, :] = tot_a[0:HALF, c] * scale
        oz[h * 10 : (h + 1) * 10, :] = tot_a[HALF:HALF_Z, c] * scale
        o1[h * HALF : (h + 1) * HALF, :] = tot_b[0:HALF, c] * scale
        oe[h * 40 : (h + 1) * 40, :] = tot_b[HALF : HALF + 40, c] * scale
    for c in started:
        c.wait_send()
    spread_sent(0, lambda to: wv.at[me], wv)
    spread_sent(1, lambda to: pb.at[to], pr)
    spread_sent(2, lambda to: rb.at[to], rr)
    spread_sent(3, lambda to: es.at[me], es)
    spread_sent(4, lambda to: nr.at[me], nr)


def vm(shape, dtype=BF):
    return pltpu.VMEM(shape, dtype)


SCRATCH = [
    vm((POS, C)), vm((POS, C)), vm((POS, C)), vm((C, C), F32),
    vm((POS + 2 * COLS, 3 * C)), vm((POS + 2 * COLS, 3 * C)), vm((POS + 2 * COLS, 3 * C)),
    vm((POS + 2 * COLS, 3 * C)), vm((POS + 2 * COLS, C)),
    vm((POS, C), F32), vm((POS, C), F32), vm((POS, C)), vm((9 * C, C)),
    vm((9 * C, C)), vm((9 * C, C)), vm((9 * C, C)), vm((9 * C, C)), vm((C, C)),
    vm((2, 8, HALF_Z, 2 * C)), vm((2, 8, HALF, 2 * C)), vm((2, 8, HALF, 2 * C)), vm((2, 8, HALF, 2 * C)),
    vm((16, 1, C), F32), vm((16, 16, 80), F32), vm((16, 16, 80), F32), vm((16, 1, 2 * C), F32),
    vm((16, 1, 2 * C), F32), vm((16, 80), F32), vm((16, 1, C), F32),
    vm((16, 1, 128), F32),
    vm((2, 8, HALF_Z, 2 * C)), vm((2, 8, HALF, 2 * C)),
    vm((8, HALF_Z, 2 * C)), vm((8, HALF, 2 * C)),
    vm((2, HALF_Z, 2 * C)), vm((2, HALF, 2 * C)),
    vm((2, 2, HALF_Z, 2 * C)), vm((2, 2, HALF, 2 * C)),
    vm((HALF_Z, 2 * C)), vm((HALF, 2 * C)),
    vm((3, HALF_Z, 2 * C)), vm((3, HALF + 40, 2 * C)),
    vm((3, HALF_Z, 2 * C)), vm((3, HALF + 40, 2 * C)),
    pltpu.SemaphoreType.DMA((4, 16)), pltpu.SemaphoreType.DMA((4, 16)),
    pltpu.SemaphoreType.DMA((5, 16)), pltpu.SemaphoreType.DMA((5, 16)),
    pltpu.SemaphoreType.DMA((2, 9)), pltpu.SemaphoreType.DMA((2, 9)),
]


def wave_of(timestep):
    half = C // 2
    freqs = jnp.exp(-math.log(10000.0) * jnp.arange(half).astype(F32) / half)
    angles = timestep.astype(F32)[:, None] * freqs[None, :]
    return jnp.concatenate([jnp.cos(angles), jnp.sin(angles)], axis=1).astype(BF).astype(F32)


def shards(
    latent, hint, timestep, skip_grad, frozen_one, frozen_two, time_weight, frozen_emb,
    train_one, train_two, train_emb, zero_weight,
):
    spec = pl.BlockSpec(memory_space=pltpu.VMEM)
    skip, g1, g2, ge, gz, norm = pl.pallas_call(
        kernel,
        out_shape=(
            jax.ShapeDtypeStruct((C, POS), BF),
            jax.ShapeDtypeStruct((180, C), F32),
            jax.ShapeDtypeStruct((180, C), F32),
            jax.ShapeDtypeStruct((80, C), F32),
            jax.ShapeDtypeStruct((20, C), F32),
            jax.ShapeDtypeStruct((1, 1), F32),
        ),
        in_specs=[spec] * 12,
        out_specs=[spec] * 6,
        scratch_shapes=SCRATCH,
        compiler_params=pltpu.CompilerParams(
            vmem_limit_bytes=67043328, collective_id=0, has_side_effects=True
        ),
    )(
        latent[0].T, hint[0].T, skip_grad[0].T, wave_of(timestep), frozen_one, frozen_two, time_weight, frozen_emb,
        train_one, train_two, train_emb, zero_weight,
    )
    return (skip.T[None], g1, g2, ge, gz, norm[0, 0])


def solution(mesh):
    data, rows_of = P(("dp", "fsdp"), None, None), P("fsdp", None)
    return jax.shard_map(
        shards,
        mesh=mesh,
        in_specs=(data, data, P(("dp", "fsdp")), data) + (rows_of,) * 8,
        out_specs=(data, rows_of, rows_of, rows_of, rows_of, P()),
        check_vma=False,
    )
```

```python
import math

import jax
import jax.numpy as jnp
from jax import lax
from jax.experimental import pallas as pl
from jax.experimental.pallas import tpu as pltpu
from jax.sharding import PartitionSpec as P

COLS = 64
POS = 1024
C = 320
TEMB = 1280
TILE = 128
STEPS = POS // TILE
MT = 256
HALF = 90
AT = 96
F32 = jnp.float32
BF = jnp.bfloat16
EPS = 1e-05
COUNT = POS * 10.0
clip_limit = 1.0
EXACT = lax.Precision.HIGHEST
MESH = pl.DeviceIdType.MESH


def rows(i, size, base=0):
    return pl.ds(pl.multiple_of(i * size + base, 16), size)


def group_matrix():
    r = lax.broadcasted_iota(jnp.int32, (C, C), 0)
    c = lax.broadcasted_iota(jnp.int32, (C, C), 1)
    return ((r * 6554) // 65536 == (c * 6554) // 65536).astype(F32).astype(BF)


def fold(x):
    return x.reshape(TILE // 8, 8, C).sum(axis=0)


def group_mean(part, g_ref):
    high = part.astype(BF)
    rest = part - high.astype(F32)
    mid = rest.astype(BF)
    low = (rest - mid.astype(F32)).astype(BF)
    split = jnp.concatenate([high, mid, low], axis=0)
    total = jnp.dot(split, g_ref[...], preferred_element_type=F32)
    return jnp.sum(total, axis=0, keepdims=True) * (1.0 / COUNT)


def stats(read, g_ref):
    zero = jnp.zeros((8, C), F32)
    mean = group_mean(lax.fori_loop(0, STEPS, lambda i, s: s + fold(read(i)), zero), g_ref)

    def square(i, s):
        d = read(i) - mean
        return s + fold(d * d)

    var = group_mean(lax.fori_loop(0, STEPS, square, zero), g_ref)
    return mean, lax.rsqrt(var + EPS)


def put_shifted(x, ref, i, order):
    j = lax.broadcasted_iota(jnp.int32, (TILE, C), 0) % COLS
    before = jnp.where(j == 0, 0.0, pltpu.roll(x, 1, 0)).astype(BF)
    after = jnp.where(j == COLS - 1, 0.0, pltpu.roll(x, TILE - 1, 0)).astype(BF)
    mid = x.astype(BF)
    parts = (before, mid, after) if order > 0 else (after, mid, before)
    ref[rows(i, TILE, COLS), :] = jnp.concatenate(parts, axis=1)


def clear_edges(ref):
    z = jnp.zeros((COLS, ref.shape[1]), ref.dtype)
    ref[0:COLS, :] = z
    ref[COLS + POS : 2 * COLS + POS, :] = z


def normed_silu(read, x3, g_ref):
    mean, inverse = stats(read, g_ref)

    def body(i, c):
        y = (read(i) - mean) * inverse
        put_shifted(y * jax.nn.sigmoid(y), x3, i, 1)
        return c

    lax.fori_loop(0, STEPS, body, 0)


def conv(x3, w_ref, write, first=0, last=POS // MT):
    def body(m, c):
        acc = None
        for a in range(3):
            t = jnp.dot(
                x3[rows(m, MT, a * COLS), :], w_ref[a * 960 : (a + 1) * 960, :], preferred_element_type=F32
            )
            acc = t if acc is None else acc + t
        write(m, acc)
        return c

    lax.fori_loop(first, last, body, 0)


def conv_back(d3, w_ref, write, first=0, last=POS // MT):
    def body(m, c):
        acc = None
        for a in range(3):
            for b in range(3):
                k = 3 * a + b
                t = lax.dot_general(
                    d3[rows(m, MT, (2 - a) * COLS), b * C : (b + 1) * C],
                    w_ref[k * C : (k + 1) * C, :],
                    (((1,), (1,)), ((), ())),
                    preferred_element_type=F32,
                )
                acc = t if acc is None else acc + t
        write(m, acc)
        return c

    lax.fori_loop(first, last, body, 0)


def turned(src, dst):
    def body(i, c):
        cols = pl.ds(pl.multiple_of(i * TILE, TILE), TILE)
        dst[rows(i, TILE), :] = src[:, cols].astype(F32).T.astype(BF)
        return c

    lax.fori_loop(0, STEPS, body, 0)


def paired(ref, dst, at, size):
    dst[at : at + size, 0:C] = ref[0:size, :]
    dst[at : at + size, C : 2 * C] = ref[size : 2 * size, :]


def add_into(dst, *others):
    total = dst[...].astype(F32)
    for o in others:
        total = total + o[...].astype(F32)
    dst[...] = total.astype(BF)


def kernel(
    lat_h, hint_h, sg_h, wave_h, f1_h, f2_h, tw_h, fe_h, t1_h, t2_h, te_h, zw_h,
    skip_h, oa_h, ob_h, onorm_h,
    lat_t, hint_t, sg_t, wave, f1, f2, tw, fe, t1, t2, te, zw, skip, oa, ob, onorm, i_sem, o_sem,
    lat, hint, sg, g_ref, xa, xb, xf, d3, dp, dq, y1, p, ctl, dw,
    w1, w2, v1, v2, wz,
    ga, gb, gc, gd, gz,
    wv, pb, pr, rb, rr, em, es, nr,
    out_a, out_b, in_a, in_b, xp_a, xp_b, xq_a, xq_b, zb_a, zb_b, cur_a, cur_b, got_a, got_b,
    g_send, g_recv, e_send, e_recv, r_send, r_recv,
):
    me_dp, me = lax.axis_index("dp"), lax.axis_index("fsdp")
    core, zh, x = lax.rem(me, 2), lax.rem(me // 2, 2), me // 4
    y, zl = me_dp // 2, lax.rem(me_dp, 2)
    oc, oh, ol = 1 - core, 1 - zh, 1 - zl
    xr, xl, xo = lax.rem(x + 1, 4), lax.rem(x + 3, 4), lax.rem(x + 2, 4)
    y_near = y + 1 - 2 * lax.rem(y, 2)
    right = (me_dp, xr * 4 + zh * 2 + core)
    left = (me_dp, xl * 4 + zh * 2 + core)
    mate = (me_dp, x * 4 + zh * 2 + oc)
    z_b = (y * 2 + ol, x * 4 + oh * 2 + core)
    z_a = (y * 2 + ol, me)
    y_a = (y_near * 2 + zl, me)
    y_b = ((3 - y) * 2 + zl, me)

    def send(src, dst, ssem, rsem, to):
        pltpu.make_async_remote_copy(
            src_ref=src, dst_ref=dst, send_sem=ssem, recv_sem=rsem, device_id=to, device_id_type=MESH
        ).start()

    def landed(ref, rsem):
        pltpu.make_async_remote_copy(
            src_ref=ref, dst_ref=ref, send_sem=rsem, recv_sem=rsem, device_id=mate, device_id_type=MESH
        ).wait_recv()

    barrier = pltpu.get_barrier_semaphore()

    def greet(k, c):
        pl.semaphore_signal(barrier, inc=1, device_id=(me_dp, lax.rem(me + k, 16)), device_id_type=MESH)
        return c

    lax.fori_loop(1, 16, greet, 0)
    for to in (z_b, z_a, y_a, y_b):
        pl.semaphore_signal(barrier, inc=1, device_id=to, device_id_type=MESH)
    from_hbm = {}
    loads = (
        ("t1", t1_h, t1), ("zw", zw_h, zw), ("wave", wave_h, wave), ("t2", t2_h, t2), ("lat", lat_h, lat_t),
        ("f1", f1_h, f1), ("f2", f2_h, f2), ("tw", tw_h, tw), ("hint", hint_h, hint_t), ("sg", sg_h, sg_t),
        ("fe", fe_h, fe), ("te", te_h, te),
    )
    for n, (name, src, dst) in enumerate(loads):
        from_hbm[name] = pltpu.make_async_copy(src, dst, i_sem.at[n])
        from_hbm[name].start()
    gathered = (ga, gb, gc, gd, gz)
    own = x * 2 + zh
    from_hbm["t1"].wait()
    from_hbm["zw"].wait()
    paired(t1, ga.at[core, own], 0, HALF)
    paired(zw, gz.at[core, own], 0, 10)
    from_hbm["wave"].wait()
    wv[me] = wave[...]
    from_hbm["t2"].wait()
    paired(t2, gb.at[core, own], 0, HALF)
    pl.semaphore_wait(barrier, 19)

    parts = ((4, 0, 8, 10), (0, 0, 24, 48), (0, 48, 72, HALF), (1, 0, 48, HALF), (2, 0, 48, HALF), (3, 0, 48, HALF))

    def block(u, j):
        w, lo, _, hi = parts[u]
        return gathered[w].at[core, j, pl.ds(lo, hi - lo)]

    def low(u, j):
        w, lo, mid, _ = parts[u]
        return gathered[w].at[core, j, pl.ds(lo, mid - lo)]

    def high(u, j):
        w, _, mid, hi = parts[u]
        return gathered[w].at[core, j, pl.ds(mid, hi - mid)]

    def pass_on(u, j):
        send(block(u, j), block(u, j), g_send.at[u, 0], g_recv.at[u, 8], mate)

    def g1(u):
        b = block(u, own)
        send(b, b, g_send.at[u, 1], g_recv.at[u, 0], right)
        send(b, b, g_send.at[u, 1], g_recv.at[u, 1], left)
        pass_on(u, own)

    def g1z(u):
        b = block(u, own)
        send(b, b, g_send.at[u, 1], g_recv.at[u, 2], z_b)

    def g2(u):
        jl, jr, jz = xl * 2 + zh, xr * 2 + zh, x * 2 + oh
        landed(block(u, jl), g_recv.at[u, 0])
        send(low(u, jl), low(u, jl), g_send.at[u, 1], g_recv.at[u, 3], right)
        landed(block(u, jr), g_recv.at[u, 1])
        send(high(u, jr), high(u, jr), g_send.at[u, 1], g_recv.at[u, 4], left)
        landed(block(u, jz), g_recv.at[u, 2])
        send(block(u, jz), block(u, jz), g_send.at[u, 1], g_recv.at[u, 5], right)
        send(block(u, jz), block(u, jz), g_send.at[u, 1], g_recv.at[u, 6], left)
        pass_on(u, jl)
        pass_on(u, jr)
        pass_on(u, jz)

    def g3(u):
        jo, jl, jr = xo * 2 + zh, xl * 2 + oh, xr * 2 + oh
        landed(low(u, jo), g_recv.at[u, 3])
        landed(high(u, jo), g_recv.at[u, 4])
        send(block(u, jo), block(u, jo), g_send.at[u, 1], g_recv.at[u, 7], z_b)
        pass_on(u, jo)
        landed(block(u, jl), g_recv.at[u, 5])
        pass_on(u, jl)
        landed(block(u, jr), g_recv.at[u, 6])
        pass_on(u, jr)

    def g4(u):
        jz = xo * 2 + oh
        landed(block(u, jz), g_recv.at[u, 7])
        pass_on(u, jz)

    def g5(u):
        w, lo, _, hi = parts[u]
        landed(gathered[w].at[oc, :, pl.ds(lo, hi - lo)], g_recv.at[u, 8])

    def sent(ref, ssem):
        pltpu.make_async_remote_copy(
            src_ref=ref, dst_ref=ref, send_sem=ssem, recv_sem=ssem, device_id=mate, device_id_type=MESH
        ).wait_send()

    def g_sent(u):
        w, lo, _, hi = parts[u]
        r = pl.ds(lo, hi - lo)
        sent(gathered[w].at[core, :, r], g_send.at[u, 0])
        sent(gathered[w].at[core, pl.ds(0, 7), r], g_send.at[u, 1])

    def unpacked(w, full):
        g = gathered[w]
        for d in range(16):
            for h in range(2):
                full[d * 180 + h * HALF : d * 180 + (h + 1) * HALF, :] = g[
                    d % 2, d // 2, 0:HALF, h * C : (h + 1) * C
                ]

    def spread(n, src_of, dst):
        def body(k, c):
            to = lax.rem(me + k, 16)
            pltpu.make_async_remote_copy(
                src_ref=src_of(to), dst_ref=dst.at[me], send_sem=e_send.at[n], recv_sem=e_recv.at[n],
                device_id=(me_dp, to), device_id_type=MESH,
            ).start()
            return c

        lax.fori_loop(1, 16, body, 0)

    def spread_wait(n, dst):
        landed(dst.at[pl.ds(0, 15)], e_recv.at[n])

    def spread_sent(n, dst):
        sent(dst.at[pl.ds(0, 15)], e_send.at[n])

    def stacked(ref):
        return jnp.concatenate([ref[s] for s in range(16)], axis=0)

    def sum_of(ref):
        total = ref[0]
        for k in range(1, 16):
            total = total + ref[k]
        return total

    chains = (
        (out_b, in_b, xp_b, xq_b, zb_b, cur_b, got_b, 0, 48, 48),
        (out_b, in_b, xp_b, xq_b, zb_b, cur_b, got_b, 48, AT, AT + 40),
        (out_a, in_a, xp_a, xq_a, zb_a, cur_a, got_a, 0, 48, 48),
        (out_a, in_a, xp_a, xq_a, zb_a, cur_a, got_a, 48, AT + 16, AT + 16),
    )

    def packed(out):
        for d in range(16):
            for h in range(2):
                out[d % 2, d // 2, 0:HALF, h * C : (h + 1) * C] = dw[
                    d * 180 + h * HALF : d * 180 + (h + 1) * HALF, :
                ]

    def step(n, k):
        out, inn, xp, xq, zb, cur, got, lo, hi, far = chains[n]
        r = pl.ds(lo, hi - lo)
        wide = pl.ds(lo, far - lo)
        if k == 1:
            send(out.at[oc, :, r], inn.at[:, r], r_send.at[n, 0], r_recv.at[n, 0], mate)
        elif k == 2:
            landed(inn.at[:, r], r_recv.at[n, 0])
            for h in range(2):
                j = xo * 2 + h
                add_into(out.at[core, j, r], inn.at[j, r])
                send(out.at[core, j, r], xp.at[h, r], r_send.at[n, 1], r_recv.at[n, 1 + h], (right, left)[h])
            for xs in (xr, xl, x):
                for h in range(2):
                    add_into(out.at[core, xs * 2 + h, r], inn.at[xs * 2 + h, r])
        elif k == 3:
            for h in range(2):
                landed(xp.at[h, r], r_recv.at[n, 1 + h])
                xs = (xr, xl)[h]
                add_into(out.at[core, xs * 2 + h, r], xp.at[h, r])
                send(
                    out.at[core, pl.ds(xs * 2, 2), r], xq.at[h, :, r], r_send.at[n, 1], r_recv.at[n, 3 + h],
                    (right, left)[h],
                )
        elif k == 4:
            landed(xq.at[0, :, r], r_recv.at[n, 3])
            landed(xq.at[1, :, r], r_recv.at[n, 4])
            add_into(out.at[core, x * 2 + oh, r], xq.at[0, oh, r], xq.at[1, oh, r])
            send(out.at[core, x * 2 + oh, r], zb.at[r], r_send.at[n, 1], r_recv.at[n, 5], z_b)
            add_into(out.at[core, x * 2 + zh, r], xq.at[0, zh, r], xq.at[1, zh, r])
        elif k == 5:
            landed(zb.at[r], r_recv.at[n, 5])
            cur[0, lo:hi, :] = (out[core, x * 2 + zh, lo:hi, :].astype(F32) + zb[lo:hi, :].astype(F32)).astype(BF)
            send(cur.at[0, wide], got.at[0, wide], r_send.at[n, 2], r_recv.at[n, 6], z_a)
        elif k < 8:
            m = k - 6
            landed(got.at[m, wide], r_recv.at[n, 6 + m])
            cur[m + 1, lo:far, :] = (cur[m, lo:far, :].astype(F32) + got[m, lo:far, :].astype(F32)).astype(BF)
            send(
                cur.at[m + 1, wide], got.at[m + 1, wide], r_send.at[n, 2], r_recv.at[n, 7 + m], (y_a, y_b)[m]
            )
        else:
            landed(got.at[2, wide], r_recv.at[n, 8])

    def step_sent(n):
        out, inn, xp, xq, zb, cur, got, lo, hi, far = chains[n]
        sent(inn.at[:, pl.ds(lo, hi - lo)], r_send.at[n, 0])
        sent(inn.at[pl.ds(0, 7), pl.ds(lo, hi - lo)], r_send.at[n, 1])
        sent(got.at[:, pl.ds(lo, far - lo)], r_send.at[n, 2])

    def grad_dots(x3, cot, b):
        lhs = x3[COLS : COLS + POS, b * C : (b + 1) * C]
        for a in range(3):
            k = 3 * a + b
            t = lax.dot_general(
                lhs, cot[128 - 64 * a : 128 - 64 * a + POS, :], (((0,), (0,)), ((), ())), preferred_element_type=F32
            )
            dw[k * C : (k + 1) * C, :] = t.astype(BF)

    def put_p(m, acc):
        p[rows(m, MT), :] = acc

    def latent_at(i):
        return lat[rows(i, TILE), :].astype(F32)

    def mixed_at(i):
        return latent_at(i) + hint[rows(i, TILE), :].astype(F32)

    for u in range(3):
        g1(u)
        g1z(u)
    spread(0, lambda to: wv.at[me], wv)
    from_hbm["f1"].wait()
    paired(f1, gc.at[core, own], 0, HALF)
    from_hbm["f2"].wait()
    paired(f2, gd.at[core, own], 0, HALF)
    from_hbm["lat"].wait()
    turned(lat_t, lat)
    from_hbm["hint"].wait()
    turned(hint_t, hint)
    g_ref[...] = group_matrix()
    for r in (xa, xb, xf, d3, dp, dq):
        clear_edges(r)
    for out, top in ((out_a, AT + 16), (out_b, AT)):
        out[:, :, 80:top, :] = jnp.zeros((2, 8, top - 80, 2 * C), BF)
    from_hbm["sg"].wait()
    turned(sg_t, sg)
    g2(0)
    g2(1)
    normed_silu(mixed_at, xa, g_ref)
    g2(2)
    g3(0)
    spread_wait(0, wv)
    from_hbm["tw"].wait()
    pick = lax.broadcasted_iota(jnp.int32, (C, 20), 0) == me * 20 + lax.broadcasted_iota(jnp.int32, (C, 20), 1)
    mine = jnp.dot(stacked(wv).astype(BF), pick.astype(F32).astype(BF), preferred_element_type=F32).astype(BF)
    pre = jnp.dot(mine, tw[...], preferred_element_type=F32)
    for e in range(16):
        pb[e] = pre[:, e * 80 : (e + 1) * 80]
    pr[me] = pb[me]
    spread(1, lambda to: pb.at[to], pr)
    g1(3)
    g3(1)
    normed_silu(latent_at, xf, g_ref)
    g3(2)
    g1z(3)
    g4(0)
    g5(0)
    for d in range(16):
        for h in range(2):
            wz[d * 20 + h * 10 : d * 20 + (h + 1) * 10, :] = gz[d % 2, d // 2, :, h * C : (h + 1) * C]

    def dc_body(i, c):
        d = lax.dot_general(sg[rows(i, TILE), :], wz[...], (((1,), (1,)), ((), ())), preferred_element_type=F32)
        d = d.astype(BF).astype(F32)
        dp[rows(i, TILE, COLS), :] = d.astype(BF)
        put_shifted(d, d3, i, -1)
        return c

    lax.fori_loop(0, STEPS, dc_body, 0)
    g4(1)
    g4(2)
    g2(3)
    g1(4)
    g1z(4)
    spread_wait(1, pr)
    from_hbm["fe"].wait()
    from_hbm["te"].wait()
    total = sum_of(pr)
    em[...] = (total * jax.nn.sigmoid(total)).astype(BF).astype(F32)
    emb = em[...].astype(BF)
    row_f = jnp.dot(emb, fe[...], preferred_element_type=F32)
    row_t = jnp.dot(emb, te[...], preferred_element_type=F32)
    both = jnp.concatenate([row_f, row_t], axis=1)
    for s in range(16):
        rb[s] = both[s : s + 1, :]
    rr[me] = rb[me]
    spread(2, lambda to: rb.at[to], rr)
    g5(1)
    g5(2)
    unpacked(0, w1)

    conv(xa, w1, put_p, 0, 2)
    conv(xa, w1, put_p, 2, 4)
    g3(3)
    spread_wait(2, rr)
    row = sum_of(rr)
    frozen_row, train_row = row[:, 0:C], row[:, C : 2 * C]

    def p_at(i):
        return p[rows(i, TILE), :]

    def train_at(i):
        return p_at(i) + train_row

    def frozen_at(i):
        return p_at(i) + frozen_row

    mean, inverse = stats(train_at, g_ref)
    g4(3)

    def y_body(i, c):
        v = (train_at(i) - mean) * inverse
        y1[rows(i, TILE), :] = v
        put_shifted(v * jax.nn.sigmoid(v), xb, i, 1)
        return c

    lax.fori_loop(0, STEPS, y_body, 0)
    g2(4)
    g1(5)
    g1z(5)
    g5(3)
    unpacked(1, w2)
    conv_back(d3, w2, put_p, 0, 2)
    conv_back(d3, w2, put_p, 2, 4)
    g3(4)
    zero = jnp.zeros((8, C), F32)

    def dy_body(i, s):
        v = y1[rows(i, TILE), :]
        sig = jax.nn.sigmoid(v)
        dy = p_at(i) * sig * (1.0 + v * (1.0 - sig))
        p[rows(i, TILE), :] = dy
        return s[0] + fold(dy), s[1] + fold(dy * v)

    s1, s2 = lax.fori_loop(0, STEPS, dy_body, (zero, zero))
    m1, m2 = group_mean(s1, g_ref), group_mean(s2, g_ref)

    def dp_body(i, s):
        d = (p_at(i) - m1 - y1[rows(i, TILE), :] * m2) * inverse
        dq[rows(i, TILE, COLS), :] = d.astype(BF)
        return s + fold(d)

    es[me] = jnp.sum(lax.fori_loop(0, STEPS, dp_body, zero), axis=0, keepdims=True)
    spread(3, lambda to: es.at[me], es)
    grad_dots(xa, dq, 0)
    g2(5)
    grad_dots(xa, dq, 1)
    grad_dots(xa, dq, 2)
    g4(4)
    packed(out_b)
    step(0, 1)
    step(1, 1)

    grad_dots(xb, dp, 0)
    g3(5)
    grad_dots(xb, dp, 1)
    step(0, 2)
    step(1, 2)
    grad_dots(xb, dp, 2)
    packed(out_a)
    step(2, 1)

    def write_control(m, acc):
        mixed = lat[rows(m, MT), :].astype(F32) + hint[rows(m, MT), :].astype(F32)
        ctl[rows(m, MT), :] = (mixed + acc).astype(BF)

    conv(xb, w2, write_control, 0, 2)
    g4(5)
    step(0, 3)
    conv(xb, w2, write_control, 2, 3)
    step(1, 3)
    conv(xb, w2, write_control, 3, 4)
    step(2, 2)
    dz = lax.dot_general(ctl[...], sg[...], (((0,), (0,)), ((), ())), preferred_element_type=F32)
    for d in range(16):
        for h in range(2):
            at = d * 20 + h * 10
            out_a[d % 2, d // 2, AT : AT + 10, h * C : (h + 1) * C] = dz[at : at + 10, :].astype(BF)
    step(3, 1)
    g5(4)
    unpacked(2, v1)
    step(0, 4)

    conv(xf, v1, put_p, 0, 1)
    spread_wait(3, es)
    de = lax.dot_general(
        em[...], stacked(es), (((0,), (0,)), ((), ())), preferred_element_type=F32, precision=EXACT
    )
    for h in range(2):
        cur_b[0, AT : AT + 40, h * C : (h + 1) * C] = de[h * 40 : (h + 1) * 40, :].astype(BF)
    step(3, 2)
    step(1, 4)
    conv(xf, v1, put_p, 1, 2)
    step(2, 3)
    conv(xf, v1, put_p, 2, 3)
    step(0, 5)
    conv(xf, v1, put_p, 3, 4)
    step(3, 3)
    step(1, 5)
    mean_f, inverse_f = stats(frozen_at, g_ref)
    step(0, 6)
    step(2, 4)

    def frozen_body(i, c):
        v = (frozen_at(i) - mean_f) * inverse_f
        put_shifted(v * jax.nn.sigmoid(v), xf, i, 1)
        return c

    lax.fori_loop(0, STEPS, frozen_body, 0)
    g5(5)
    unpacked(3, v2)
    step(1, 6)

    def write_skip(m, acc):
        out = lat[rows(m, MT), :].astype(F32) + acc
        out = out + jnp.dot(ctl[rows(m, MT), :], wz[...], preferred_element_type=F32)
        skip[:, pl.ds(pl.multiple_of(m * MT, MT), MT)] = out.T.astype(BF)

    conv(xf, v2, write_skip, 0, 1)
    step(0, 7)
    step(2, 5)
    conv(xf, v2, write_skip, 1, 2)
    step(3, 4)
    step(1, 7)
    conv(xf, v2, write_skip, 2, 3)
    step(2, 6)
    conv(xf, v2, write_skip, 3, 4)
    skip_out = pltpu.make_async_copy(skip, skip_h, o_sem.at[0])
    skip_out.start()
    step(3, 5)
    step(2, 7)
    step(3, 6)
    step(3, 7)
    for n in range(4):
        step(n, 8)
    tot_a = cur_a[2].astype(F32) + got_a[2].astype(F32)
    tot_b = cur_b[2].astype(F32) + got_b[2].astype(F32)
    row_at = lax.broadcasted_iota(jnp.int32, (AT + 40, 2 * C), 0)
    own_a = jnp.where((row_at < HALF) | ((row_at >= AT) & (row_at < AT + 10)), jnp.pad(tot_a, ((0, 24), (0, 0))), 0.0)
    own_b = jnp.where((row_at < HALF) | (row_at >= AT), tot_b, 0.0)
    sq = jnp.sum(own_a * own_a, axis=0, keepdims=True) + jnp.sum(own_b * own_b, axis=0, keepdims=True)
    nr[me] = jnp.broadcast_to(jnp.sum(sq, axis=1, keepdims=True), (1, 128))
    spread(4, lambda to: nr.at[me], nr)
    for u in range(6):
        g_sent(u)
    for n in range(4):
        step_sent(n)
    spread_sent(0, wv)
    spread_sent(1, pr)
    spread_sent(2, rr)
    spread_sent(3, es)
    skip_out.wait()
    spread_wait(4, nr)
    norm = jnp.sqrt(sum_of(nr)[:, 0:1] + 1e-06)
    scale = jnp.minimum(1.0, clip_limit / norm)
    onorm[...] = jnp.broadcast_to(norm, (8, 128))
    oa[...] = tot_a * scale
    ob[...] = tot_b * scale
    results = []
    for n, (src, dst) in enumerate(((oa, oa_h), (ob, ob_h), (onorm, onorm_h))):
        results.append(pltpu.make_async_copy(src, dst, o_sem.at[n + 1]))
        results[-1].start()
    for c in results:
        c.wait()
    spread_sent(4, nr)


def vm(shape, dtype=BF):
    return pltpu.VMEM(shape, dtype)


SCRATCH = [
    vm((C, POS)), vm((C, POS)), vm((C, POS)), vm((1, C), F32), vm((180, C)), vm((180, C)), vm((20, TEMB)),
    vm((80, C)), vm((180, C)), vm((180, C)), vm((80, C)), vm((20, C)),
    vm((C, POS)), vm((AT + 16, 2 * C), F32), vm((AT + 40, 2 * C), F32), vm((8, 128), F32),
    pltpu.SemaphoreType.DMA((12,)), pltpu.SemaphoreType.DMA((4,)),
    vm((POS, C)), vm((POS, C)), vm((POS, C)), vm((C, C)),
    vm((POS + 2 * COLS, 3 * C)), vm((POS + 2 * COLS, 3 * C)), vm((POS + 2 * COLS, 3 * C)),
    vm((POS + 2 * COLS, 3 * C)), vm((POS + 2 * COLS, C)), vm((POS + 2 * COLS, C)),
    vm((POS, C), F32), vm((POS, C), F32), vm((POS, C)), vm((9 * C, C)),
    vm((9 * C, C)), vm((9 * C, C)), vm((9 * C, C)), vm((9 * C, C)), vm((C, C)),
    vm((2, 8, HALF, 2 * C)), vm((2, 8, HALF, 2 * C)), vm((2, 8, HALF, 2 * C)), vm((2, 8, HALF, 2 * C)),
    vm((2, 8, 10, 2 * C)),
    vm((16, 1, C), F32), vm((16, 16, 80), F32), vm((16, 16, 80), F32), vm((16, 1, 2 * C), F32),
    vm((16, 1, 2 * C), F32), vm((16, 80), F32), vm((16, 1, C), F32),
    vm((16, 1, 128), F32),
    vm((2, 8, AT + 16, 2 * C)), vm((2, 8, AT, 2 * C)),
    vm((8, AT + 16, 2 * C)), vm((8, AT, 2 * C)),
    vm((2, AT + 16, 2 * C)), vm((2, AT, 2 * C)),
    vm((2, 2, AT + 16, 2 * C)), vm((2, 2, AT, 2 * C)),
    vm((AT + 16, 2 * C)), vm((AT, 2 * C)),
    vm((3, AT + 16, 2 * C)), vm((3, AT + 40, 2 * C)),
    vm((3, AT + 16, 2 * C)), vm((3, AT + 40, 2 * C)),
    pltpu.SemaphoreType.DMA((6, 2)), pltpu.SemaphoreType.DMA((6, 9)),
    pltpu.SemaphoreType.DMA((5,)), pltpu.SemaphoreType.DMA((5,)),
    pltpu.SemaphoreType.DMA((4, 3)), pltpu.SemaphoreType.DMA((4, 9)),
]


def finish(skip_in, a_in, b_in, n_in, skip_out, o1_h, o2_h, oe_h, oz_h, on_h, sk, a, b, nv, o1, o2, oe, oz, on, i_sem, o_sem):
    loads = [
        pltpu.make_async_copy(src, dst, i_sem.at[n])
        for n, (src, dst) in enumerate(((skip_in, sk), (a_in, a), (b_in, b), (n_in, nv)))
    ]
    for c in loads:
        c.start()
    stores = []

    def put(src, dst):
        stores.append(pltpu.make_async_copy(src, dst, o_sem.at[len(stores)]))
        stores[-1].start()

    loads[0].wait()
    put(sk, skip_out)
    for c in loads[1:]:
        c.wait()
    for h in range(2):
        c = slice(h * C, (h + 1) * C)
        o2[h * HALF : (h + 1) * HALF, :] = a[0:HALF, c]
        oz[h * 10 : (h + 1) * 10, :] = a[AT : AT + 10, c]
        o1[h * HALF : (h + 1) * HALF, :] = b[0:HALF, c]
        oe[h * 40 : (h + 1) * 40, :] = b[AT : AT + 40, c]
    on[...] = nv[0:1, 0:1]
    for src, dst in ((o1, o1_h), (o2, o2_h), (oe, oe_h), (oz, oz_h), (on, on_h)):
        put(src, dst)
    for c in stores:
        c.wait()


def wave_of(timestep):
    half = C // 2
    freqs = jnp.exp(-math.log(10000.0) * jnp.arange(half).astype(F32) / half)
    angles = timestep.astype(F32)[:, None] * freqs[None, :]
    return jnp.concatenate([jnp.cos(angles), jnp.sin(angles)], axis=1).astype(BF).astype(F32)


def shards(
    latent, hint, timestep, skip_grad, frozen_one, frozen_two, time_weight, frozen_emb,
    train_one, train_two, train_emb, zero_weight,
):
    spec = pl.BlockSpec(memory_space=pl.ANY)
    held = pl.pallas_call(
        kernel,
        out_shape=(
            jax.ShapeDtypeStruct((C, POS), BF),
            jax.ShapeDtypeStruct((AT + 16, 2 * C), F32),
            jax.ShapeDtypeStruct((AT + 40, 2 * C), F32),
            jax.ShapeDtypeStruct((8, 128), F32),
        ),
        in_specs=[spec] * 12,
        out_specs=[spec] * 4,
        scratch_shapes=SCRATCH,
        compiler_params=pltpu.CompilerParams(
            vmem_limit_bytes=67043328, collective_id=0, has_side_effects=True
        ),
    )(
        latent[0].T, hint[0].T, skip_grad[0].T, wave_of(timestep), frozen_one, frozen_two, time_weight, frozen_emb,
        train_one, train_two, train_emb, zero_weight,
    )
    skip, g1, g2, ge, gz, norm = pl.pallas_call(
        finish,
        out_shape=(
            jax.ShapeDtypeStruct((C, POS), BF),
            jax.ShapeDtypeStruct((180, C), F32),
            jax.ShapeDtypeStruct((180, C), F32),
            jax.ShapeDtypeStruct((80, C), F32),
            jax.ShapeDtypeStruct((20, C), F32),
            jax.ShapeDtypeStruct((1, 1), F32),
        ),
        in_specs=[pl.BlockSpec(memory_space=pltpu.HBM)] * 4,
        out_specs=[spec] * 6,
        scratch_shapes=[
            vm((C, POS)), vm((AT + 16, 2 * C), F32), vm((AT + 40, 2 * C), F32), vm((8, 128), F32),
            vm((180, C), F32), vm((180, C), F32), vm((80, C), F32), vm((20, C), F32), vm((1, 1), F32),
            pltpu.SemaphoreType.DMA((4,)), pltpu.SemaphoreType.DMA((6,)),
        ],
        compiler_params=pltpu.CompilerParams(vmem_limit_bytes=67043328),
    )(*held)
    return (skip.T[None], g1, g2, ge, gz, norm[0, 0])


def solution(mesh):
    data, rows_of = P(("dp", "fsdp"), None, None), P("fsdp", None)
    return jax.shard_map(
        shards,
        mesh=mesh,
        in_specs=(data, data, P(("dp", "fsdp")), data) + (rows_of,) * 8,
        out_specs=(data, rows_of, rows_of, rows_of, rows_of, P()),
        check_vma=False,
    )
```
